32 devices in a mesh: dp: 1 (over z), tp: 32 (over y, x, core).
Axes of the slice: x: 4, y: 4, z: 1, core: 2. Of those that a mesh axis runs over, the one named last changes fastest.
The devices are a block of a 4x4x8 slice.
Arguments:
- X: bfloat16 [256, 4096], P('dp')
- W: bfloat16 [4096, 32768], P(None, 'tp')
- labels: int32 [256], P('dp')
Outputs:
- output 1: float32 [1], P('dp')
- output 2: bfloat16 [4096, 32768], P('dp', 'tp')
- output 3: bfloat16 [256, 4096], P('dp')
All inputs are finite; a program needn't handle non-finite values.
Results may differ from the reference program's by a relative error of at most 0.001.
Values are sent between devices in bfloat16 or wider.
A program may use at most 768 MiB of HBM per device.

```python
import math

import jax
import jax.numpy as jnp
from jax import lax

T = 256
H = 4096
V = 32768


def setup_inputs(seed: int = 0, part: int = 0) -> dict:
    key = jax.random.PRNGKey(seed)
    kshared, kpart = jax.random.split(key)
    kp = jax.random.fold_in(kpart, part)
    kx, kl, kc, ku, kv, kg = jax.random.split(kp, 6)
    nb = 4
    Wf = jax.random.normal(kshared, (H, V), jnp.float32) * H ** -0.5
    kl1, kl2 = jax.random.split(jax.random.fold_in(kl, 7))
    la = jax.random.randint(kl1, (T,), 0, V // 16, jnp.int32)
    lb = jax.random.randint(kl2, (T,), 0, V, jnp.int32)
    labels = jnp.where(jnp.arange(T) % 2 == 0, la, lb)
    cols = jax.random.randint(kc, (T, nb), 0, V, jnp.int32)
    amp = math.log(V) + jax.random.uniform(ku, (T, nb), jnp.float32, 0.0, 2.5)
    amp_label = (math.log(V) + jax.random.uniform(kv, (T,), jnp.float32, -2.0, 2.0)
                 + jax.random.uniform(kg, (), jnp.float32, -1.0, 1.0))
    X = jax.random.normal(kx, (T, H), jnp.float32)
    for k in range(nb):
        X = X + amp[:, k:k + 1] * Wf[:, cols[:, k]].T
    X = X + amp_label[:, None] * Wf[:, labels].T
    return {'X': X.astype(jnp.bfloat16), 'W': Wf.astype(jnp.bfloat16), 'labels': labels}


def reference(X, W, labels):
    VC = min(V, 2048)
    nb = V // VC
    Wb = W.reshape(H, nb, VC).transpose(1, 0, 2)
    offs = jnp.arange(nb, dtype=jnp.int32) * VC
    cols = jnp.arange(VC, dtype=jnp.int32)

    def stats(a):
        w, off = a
        z = jnp.dot(X, w, preferred_element_type=jnp.float32)
        m = z.max(axis=1)
        s = jnp.exp(z - m[:, None]).sum(axis=1)
        hit = (cols[None, :] + off) == labels[:, None]
        t = jnp.where(hit, z, 0.0).sum(axis=1)
        return m, s, t

    m, s, t = lax.map(stats, (Wb, offs))
    M = m.max(axis=0)
    S = (s * jnp.exp(m - M[None, :])).sum(axis=0)
    zt = t.sum(axis=0)
    L = jnp.mean(M + jnp.log(S) - zt).reshape(1)

    def back(dx, a):
        w, off = a
        z = jnp.dot(X, w, preferred_element_type=jnp.float32)
        hit = (cols[None, :] + off) == labels[:, None]
        g = ((jnp.exp(z - M[:, None]) / S[:, None] - hit.astype(jnp.float32)) / T).astype(jnp.bfloat16)
        dw = jnp.dot(X.T, g, preferred_element_type=jnp.float32).astype(jnp.bfloat16)
        dx = dx + jnp.dot(g, w.T, preferred_element_type=jnp.float32)
        return dx, dw

    dx, dWb = lax.scan(back, jnp.zeros((T, H), jnp.float32), (Wb, offs))
    dW = dWb.transpose(1, 0, 2).reshape(H, V)
    return (L, dW, dx.astype(jnp.bfloat16))
```

```python
import functools
import math

import jax
import jax.numpy as jnp
from jax import lax
from jax.experimental import pallas as pl
from jax.experimental.pallas import tpu as pltpu
from jax.sharding import PartitionSpec as P

MESH = pl.DeviceIdType.MESH
F32 = jnp.float32
BF16 = jnp.bfloat16
LANES = 128
CORES = 2
NT = (((1,), (1,)), ((), ()))
TN = (((0,), (0,)), ((), ()))


def head_kernel(n_dev, side, X_hbm, W_hbm, lab_ref, L_ref, G_hbm, DX_hbm,
                x_v, w_v, z_v, lab_v, st_v, f_v, msg_v, all_v, g_v,
                own, ds, dr, r1, r2, q_v, t1, t2, dx_v,
                in_sem, w_sem, st_ssem, st_rsem, ssem, rsem, out_sem):
    T, H = x_v.shape
    V = w_v.shape[1]
    R = T // 2
    HC = H // CORES
    U = HC // side
    UH = U // 2
    J = U // side
    RH = R // 2

    me = lax.axis_index('tp')
    c = lax.rem(me, CORES)
    x = lax.rem(me // CORES, side)
    y = me // (CORES * side)
    partner = me + 1 - 2 * c

    def dev(yy, xx):
        return (yy * side + xx) * CORES + c

    def wrap(a):
        return lax.rem(a, side)

    first = (x, y)
    second = (y, x)

    def near1(s, d):
        return dev(y, wrap(x + d)) if s == 0 else dev(wrap(y + d), x)

    def near2(s, d):
        return dev(wrap(y + d), x) if s == 0 else dev(y, wrap(x + d))

    barrier = pltpu.get_barrier_semaphore()

    def greet(i, carry):
        pl.semaphore_signal(barrier, inc=1, device_id={'tp': lax.rem(me + 1 + i, n_dev)}, device_id_type=MESH)
        return carry

    lax.fori_loop(0, n_dev - 1, greet, 0)

    NB = w_sem.shape[0]
    VB = V // NB
    x_in = pltpu.make_async_copy(X_hbm, x_v, in_sem.at[0])
    x_in.start()

    def w_in(i):
        cols = pl.ds(pl.multiple_of(i * VB, VB), VB)
        return pltpu.make_async_copy(W_hbm.at[:, cols], w_v.at[:, cols], w_sem.at[i])

    for i in range(NB):
        w_in(i).start()

    labf = lab_ref[...].astype(F32)
    for b in range(T // LANES):
        row = labf[:, b * LANES:(b + 1) * LANES]
        lab_v[b * LANES:(b + 1) * LANES, :] = jnp.broadcast_to(row, (LANES, LANES)).T

    x_in.wait()

    def logits(i, carry):
        w_in(i).wait()
        cols = pl.ds(pl.multiple_of(i * VB, VB), VB)
        z_v[:, cols] = jnp.dot(x_v[...], w_v[:, cols], preferred_element_type=F32)
        return carry

    lax.fori_loop(0, NB, logits, 0)

    SB = 32
    base = (me * V).astype(F32)
    cols_f = lax.broadcasted_iota(jnp.int32, (SB, V), 1).astype(F32) + base
    lane = lax.broadcasted_iota(jnp.int32, (SB, LANES), 1)

    def stats(i, carry):
        r = pl.ds(pl.multiple_of(i * SB, SB), SB)
        z = z_v[r, :]
        m = jnp.max(z, axis=1, keepdims=True)
        e = jnp.exp(z - m)
        s = jnp.sum(e, axis=1, keepdims=True)
        zt = jnp.sum(jnp.where(cols_f == lab_v[r, 0:1], z, 0.0), axis=1, keepdims=True)
        z_v[r, :] = e
        ln = lane - 4 * (i // (LANES // SB))
        st_v[r, :] = jnp.where(ln == 0, m, jnp.where(ln == 1, s, jnp.where(ln == 2, zt, 0.0)))
        return carry

    lax.fori_loop(0, T // SB, stats, 0)
    msg = st_v[0:LANES, :].T[0:8, :] + st_v[LANES:2 * LANES, :].T[0:8, :]
    msg_v[...] = msg
    all_v[pl.ds(me, 1)] = msg[None]

    pl.semaphore_wait(barrier, n_dev - 1)

    def send_stats(i, carry):
        pltpu.make_async_remote_copy(
            src_ref=msg_v, dst_ref=all_v.at[me], send_sem=st_ssem, recv_sem=st_rsem,
            device_id={'tp': lax.rem(me + 1 + i, n_dev)}, device_id_type=MESH).start()
        return carry

    lax.fori_loop(0, n_dev - 1, send_stats, 0)
    rest = all_v.at[pl.ds(0, n_dev - 1)]
    everybody = pltpu.make_async_remote_copy(
        src_ref=rest, dst_ref=rest, send_sem=st_ssem, recv_sem=st_rsem,
        device_id={'tp': partner}, device_id_type=MESH)
    everybody.wait_recv()

    loss = jnp.zeros((1, 1), F32)
    for b in range(T // LANES):
        m = all_v[:, 4 * b, :]
        s = all_v[:, 4 * b + 1, :]
        zt = jnp.sum(all_v[:, 4 * b + 2, :], axis=0, keepdims=True)
        M = jnp.max(m, axis=0, keepdims=True)
        S = jnp.sum(s * jnp.exp(m - M), axis=0, keepdims=True)
        loss = loss + jnp.sum(M + jnp.log(S) - zt, axis=1, keepdims=True)
        f = jnp.exp(msg_v[4 * b:4 * b + 1, :] - M) / (S * T)
        f_v[b * LANES:(b + 1) * LANES, :] = jnp.broadcast_to(f, (LANES, LANES)).T
    L_ref[...] = loss / T

    def grads(i, carry):
        r = pl.ds(pl.multiple_of(i * SB, SB), SB)
        hit = jnp.where(cols_f == lab_v[r, 0:1], 1.0 / T, 0.0)
        g_v[r, :] = (z_v[r, :] * f_v[r, 0:1] - hit).astype(BF16)
        return carry

    lax.fori_loop(0, T // SB, grads, 0)
    g_out = pltpu.make_async_copy(g_v, G_hbm, out_sem.at[0])
    g_out.start()

    sent = []

    def rcopy(src, dst, to):
        i = len(sent)
        d = pltpu.make_async_remote_copy(src_ref=src, dst_ref=dst, send_sem=ssem.at[i], recv_sem=rsem.at[i],
                                         device_id={'tp': to}, device_id_type=MESH)
        d.start()
        sent.append(d)
        return d

    def unit(k, lo=0, n=U):
        return pl.ds(pl.multiple_of(k * U + lo, LANES), n)

    def part(s, k, core):
        wr = pl.ds(pl.multiple_of(core * HC + k * U, U), U)
        return lax.dot_general(g_v[s * R:(s + 1) * R, :], w_v[wr, :], NT, preferred_element_type=F32)

    pair = {}

    def produce(off):
        for s in (0, 1):
            k = wrap(first[s] + off)
            ds[s, :, unit(k)] = part(s, k, 1 - c)
            pair[s, off] = rcopy(ds.at[s, :, unit(k)], dr.at[s, :, unit(k)], partner)
        for s in (0, 1):
            k = wrap(first[s] + off)
            own[s, :, unit(k)] = part(s, k, c)

    def join(s, off):
        k = wrap(first[s] + off)
        pair[s, off].wait_recv()
        own[s, :, unit(k)] += dr[s, :, unit(k)]

    one = {}
    produce(2)
    produce(1)
    for s in (0, 1):
        join(s, 2)
        k = wrap(first[s] + 2)
        one[s, 0] = rcopy(own.at[s, :, unit(k, 0, UH)], r1.at[s, 0], near1(s, 1))
        one[s, 1] = rcopy(own.at[s, :, unit(k, UH, UH)], r1.at[s, 1], near1(s, side - 1))
    produce(3)
    for s in (0, 1):
        join(s, 1)
        k = wrap(first[s] + 1)
        one[s, 2] = rcopy(own.at[s, :, unit(k, UH, UH)], r2.at[s, 0, :, UH:U], near1(s, 1))
    produce(0)
    for s in (0, 1):
        join(s, 3)
        k = wrap(first[s] + 3)
        one[s, 3] = rcopy(own.at[s, :, unit(k, 0, UH)], r2.at[s, 1, :, 0:UH], near1(s, side - 1))
    for s in (0, 1):
        join(s, 0)
    for s in (0, 1):
        kp = wrap(first[s] + 1)
        km = wrap(first[s] + 3)
        one[s, 0].wait_recv()
        own[s, :, unit(kp, 0, UH)] += r1[s, 0]
        one[s, 4] = rcopy(own.at[s, :, unit(kp, 0, UH)], r2.at[s, 0, :, 0:UH], near1(s, 1))
        one[s, 1].wait_recv()
        own[s, :, unit(km, UH, UH)] += r1[s, 1]
        one[s, 5] = rcopy(own.at[s, :, unit(km, UH, UH)], r2.at[s, 1, :, UH:U], near1(s, side - 1))

    def col2(j):
        return pl.ds(pl.multiple_of(j * J, LANES), J)

    two = {}
    top, bot = slice(0, RH), slice(RH, R)
    for s in (0, 1):
        for i in (2, 3, 4, 5):
            one[s, i].wait_recv()
        q_v[s] = own[s, :, unit(first[s])] + r2[s, 0] + r2[s, 1]
        jo, jp, jm = (wrap(second[s] + d) for d in (2, 1, 3))
        two[s, 0] = rcopy(q_v.at[s, top, col2(jo)], t1.at[s, 0], near2(s, 1))
        two[s, 1] = rcopy(q_v.at[s, bot, col2(jo)], t1.at[s, 1], near2(s, side - 1))
        two[s, 2] = rcopy(q_v.at[s, bot, col2(jp)], t2.at[s, 0, bot], near2(s, 1))
        two[s, 3] = rcopy(q_v.at[s, top, col2(jm)], t2.at[s, 1, top], near2(s, side - 1))
    for s in (0, 1):
        jp, jm = (wrap(second[s] + d) for d in (1, 3))
        two[s, 0].wait_recv()
        q_v[s, top, col2(jp)] += t1[s, 0]
        two[s, 4] = rcopy(q_v.at[s, top, col2(jp)], t2.at[s, 0, top], near2(s, 1))
        two[s, 1].wait_recv()
        q_v[s, bot, col2(jm)] += t1[s, 1]
        two[s, 5] = rcopy(q_v.at[s, bot, col2(jm)], t2.at[s, 1, bot], near2(s, side - 1))

    def at2(s, j, half):
        rows = slice(s * R + half * RH, s * R + (half + 1) * RH)
        return dx_v.at[rows, pl.ds(pl.multiple_of(c * HC + first[s] * U + j * J, LANES), J)]

    def at1(s, k, half):
        return dx_v.at[s * R:(s + 1) * R, pl.ds(pl.multiple_of(c * HC + k * U + half * UH, LANES), UH)]

    def block(s, k):
        return pl.ds(pl.multiple_of(c * HC + k * U, LANES), U)

    three = {}
    for s in (0, 1):
        j = second[s]
        for i in (2, 3, 4, 5):
            two[s, i].wait_recv()
        total = q_v[s, :, col2(j)] + t2[s, 0] + t2[s, 1]
        dx_v[s * R:(s + 1) * R, pl.ds(pl.multiple_of(c * HC + first[s] * U + j * J, LANES), J)] = total.astype(BF16)
        three[s, 0] = rcopy(at2(s, j, 0), at2(s, j, 0), near2(s, 1))
        three[s, 1] = rcopy(at2(s, j, 1), at2(s, j, 1), near2(s, side - 1))
        three[s, 2] = rcopy(at2(s, j, 1), at2(s, j, 1), near2(s, 1))
        three[s, 3] = rcopy(at2(s, j, 0), at2(s, j, 0), near2(s, side - 1))
    for s in (0, 1):
        jp, jm = (wrap(second[s] + d) for d in (1, 3))
        three[s, 0].wait_recv()
        three[s, 4] = rcopy(at2(s, jm, 0), at2(s, jm, 0), near2(s, 1))
        three[s, 1].wait_recv()
        three[s, 5] = rcopy(at2(s, jp, 1), at2(s, jp, 1), near2(s, side - 1))

    outs = []

    def put(s, cols):
        d = pltpu.make_async_copy(dx_v.at[s * R:(s + 1) * R, cols], DX_hbm.at[s * R:(s + 1) * R, cols],
                                  out_sem.at[1 + len(outs)])
        d.start()
        outs.append(d)

    four = {}
    pairs = []

    def share(s, k):
        ref = dx_v.at[s * R:(s + 1) * R, block(s, k)]
        pairs.append((s, k, rcopy(ref, ref, partner)))
        put(s, block(s, k))

    for s in (0, 1):
        for i in (2, 3, 4, 5):
            three[s, i].wait_recv()
        k = first[s]
        four[s, 0] = rcopy(at1(s, k, 0), at1(s, k, 0), near1(s, 1))
        four[s, 1] = rcopy(at1(s, k, 1), at1(s, k, 1), near1(s, side - 1))
        four[s, 2] = rcopy(at1(s, k, 1), at1(s, k, 1), near1(s, 1))
        four[s, 3] = rcopy(at1(s, k, 0), at1(s, k, 0), near1(s, side - 1))
        share(s, k)
    for s in (0, 1):
        kp, km = (wrap(first[s] + d) for d in (1, 3))
        four[s, 0].wait_recv()
        four[s, 4] = rcopy(at1(s, km, 0), at1(s, km, 0), near1(s, 1))
        four[s, 1].wait_recv()
        four[s, 5] = rcopy(at1(s, kp, 1), at1(s, kp, 1), near1(s, side - 1))
    for s in (0, 1):
        four[s, 2].wait_recv()
        share(s, wrap(first[s] + 3))
        four[s, 3].wait_recv()
        share(s, wrap(first[s] + 1))
    for s in (0, 1):
        four[s, 4].wait_recv()
        four[s, 5].wait_recv()
        share(s, wrap(first[s] + 2))
    for s, k, d in pairs:
        d.wait_recv()
        put(s, pl.ds(pl.multiple_of((1 - c) * HC + k * U, LANES), U))

    everybody.wait_send()
    for d in sent:
        d.wait_send()
    g_out.wait()
    for d in outs:
        d.wait()


N_COPIES = 8 + 4 * 12 + 8
N_OUTS = 1 + 16


def dw_kernel(x_ref, g_ref, o_ref):
    o_ref[...] = lax.dot_general(x_ref[...], g_ref[...], TN, preferred_element_type=F32).astype(BF16)


def solution(mesh):
    n_dev = mesh.shape['tp']
    side = math.isqrt(n_dev // CORES)

    def local(X, W, labels):
        T, H = X.shape
        V = W.shape[1]
        R, HC = T // 2, H // CORES
        U = HC // side
        J = U // side
        any_ = pl.BlockSpec(memory_space=pl.ANY)
        vmem = pl.BlockSpec(memory_space=pltpu.VMEM)
        L, G, dX = pl.pallas_call(
            functools.partial(head_kernel, n_dev, side),
            name='head',
            out_shape=(jax.ShapeDtypeStruct((1, 1), F32), jax.ShapeDtypeStruct((T, V), BF16),
                       jax.ShapeDtypeStruct((T, H), BF16)),
            in_specs=[any_, any_, vmem],
            out_specs=(vmem, any_, any_),
            scratch_shapes=[
                pltpu.VMEM((T, H), BF16), pltpu.VMEM((H, V), BF16), pltpu.VMEM((T, V), F32),
                pltpu.VMEM((T, LANES), F32), pltpu.VMEM((T, LANES), F32), pltpu.VMEM((T, LANES), F32),
                pltpu.VMEM((8, LANES), F32), pltpu.VMEM((n_dev, 8, LANES), F32), pltpu.VMEM((T, V), BF16),
                pltpu.VMEM((2, R, HC), F32), pltpu.VMEM((2, R, HC), F32), pltpu.VMEM((2, R, HC), F32),
                pltpu.VMEM((2, 2, R, U // 2), F32), pltpu.VMEM((2, 2, R, U), F32), pltpu.VMEM((2, R, U), F32),
                pltpu.VMEM((2, 2, R // 2, J), F32), pltpu.VMEM((2, 2, R, J), F32), pltpu.VMEM((T, H), BF16),
                pltpu.SemaphoreType.DMA((1,)), pltpu.SemaphoreType.DMA((4,)),
                pltpu.SemaphoreType.DMA, pltpu.SemaphoreType.DMA,
                pltpu.SemaphoreType.DMA((N_COPIES,)), pltpu.SemaphoreType.DMA((N_COPIES,)),
                pltpu.SemaphoreType.DMA((N_OUTS,)),
            ],
            compiler_params=pltpu.CompilerParams(collective_id=0, has_side_effects=True,
                                                 vmem_limit_bytes=48 * 1024 * 1024),
        )(X, W, labels.reshape(1, T))

        HB = H // 8
        dW = pl.pallas_call(
            dw_kernel,
            name='dw',
            out_shape=jax.ShapeDtypeStruct((H, V), BF16),
            grid=(H // HB,),
            in_specs=[pl.BlockSpec((T, HB), lambda i: (0, i)), pl.BlockSpec((T, V), lambda i: (0, 0))],
            out_specs=pl.BlockSpec((HB, V), lambda i: (i, 0)),
            compiler_params=pltpu.CompilerParams(dimension_semantics=('arbitrary',)),
        )(X, G)
        return L.reshape(1), dW, dX

    return jax.shard_map(local, mesh=mesh,
                         in_specs=(P('dp', None), P(None, 'tp'), P('dp')),
                         out_specs=(P('dp'), P('dp', 'tp'), P('dp', None)),
                         check_vma=False)
```

```python
import functools
import math

import jax
import jax.numpy as jnp
from jax import lax
from jax.experimental import pallas as pl
from jax.experimental.pallas import tpu as pltpu
from jax.sharding import PartitionSpec as P

MESH = pl.DeviceIdType.MESH
F32 = jnp.float32
BF16 = jnp.bfloat16
LANES = 128
CORES = 2
NT = (((1,), (1,)), ((), ()))
TN = (((0,), (0,)), ((), ()))


def head_kernel(n_dev, side, X_hbm, W_hbm, lab_hbm, L_ref, dw_v, dx_v,
                x_v, w_v, xt_v, z_v, labr_v, lab_v, st_v, f_v, msg_v, all_v, g_v,
                own, ds, dr, r1, r2, q_v, t1, t2,
                in_sem, w_sem, st_ssem, st_rsem, ssem, rsem):
    T, H = x_v.shape
    V = w_v.shape[1]
    R = T // 2
    HC = H // CORES
    U = HC // side
    UH = U // 2
    J = U // side
    RH = R // 2

    me = lax.axis_index('tp')
    c = lax.rem(me, CORES)
    x = lax.rem(me // CORES, side)
    y = me // (CORES * side)
    partner = me + 1 - 2 * c

    def dev(yy, xx):
        return (yy * side + xx) * CORES + c

    def wrap(a):
        return lax.rem(a, side)

    first = (x, y)
    second = (y, x)

    def near1(s, d):
        return dev(y, wrap(x + d)) if s == 0 else dev(wrap(y + d), x)

    def near2(s, d):
        return dev(wrap(y + d), x) if s == 0 else dev(y, wrap(x + d))

    barrier = pltpu.get_barrier_semaphore()

    def greet(i, carry):
        pl.semaphore_signal(barrier, inc=1, device_id={'tp': lax.rem(me + 1 + i, n_dev)}, device_id_type=MESH)
        return carry

    lax.fori_loop(0, n_dev - 1, greet, 0)

    NB = w_sem.shape[0]
    VB = V // NB
    x_in = pltpu.make_async_copy(X_hbm, x_v, in_sem.at[0])
    x_in.start()
    lab_in = pltpu.make_async_copy(lab_hbm, labr_v, in_sem.at[1])
    lab_in.start()

    def w_in(i):
        cols = pl.ds(pl.multiple_of(i * VB, VB), VB)
        return pltpu.make_async_copy(W_hbm.at[:, cols], w_v.at[:, cols], w_sem.at[i])

    for i in range(NB):
        w_in(i).start()

    lab_in.wait()
    labf = labr_v[...].astype(F32)
    for b in range(T // LANES):
        row = labf[:, b * LANES:(b + 1) * LANES]
        lab_v[b * LANES:(b + 1) * LANES, :] = jnp.broadcast_to(row, (LANES, LANES)).T

    x_in.wait()

    def logits(i, carry):
        w_in(i).wait()
        cols = pl.ds(pl.multiple_of(i * VB, VB), VB)
        z_v[:, cols] = jnp.dot(x_v[...], w_v[:, cols], preferred_element_type=F32)
        return carry

    lax.fori_loop(0, NB, logits, 0)

    SB = 32
    base = (me * V).astype(F32)
    cols_f = lax.broadcasted_iota(jnp.int32, (SB, V), 1).astype(F32) + base
    lane = lax.broadcasted_iota(jnp.int32, (SB, LANES), 1)

    def stats(i, carry):
        r = pl.ds(pl.multiple_of(i * SB, SB), SB)
        z = z_v[r, :]
        m = jnp.max(z, axis=1, keepdims=True)
        e = jnp.exp(z - m)
        s = jnp.sum(e, axis=1, keepdims=True)
        zt = jnp.sum(jnp.where(cols_f == lab_v[r, 0:1], z, 0.0), axis=1, keepdims=True)
        z_v[r, :] = e
        ln = lane - 4 * (i // (LANES // SB))
        st_v[r, :] = jnp.where(ln == 0, m, jnp.where(ln == 1, s, jnp.where(ln == 2, zt, 0.0)))
        return carry

    lax.fori_loop(0, T // SB, stats, 0)
    msg = st_v[0:LANES, :].T[0:8, :] + st_v[LANES:2 * LANES, :].T[0:8, :]
    msg_v[...] = msg
    all_v[pl.ds(me, 1)] = msg[None]

    pl.semaphore_wait(barrier, n_dev - 1)

    def send_stats(i, carry):
        pltpu.make_async_remote_copy(
            src_ref=msg_v, dst_ref=all_v.at[me], send_sem=st_ssem, recv_sem=st_rsem,
            device_id={'tp': lax.rem(me + 1 + i, n_dev)}, device_id_type=MESH).start()
        return carry

    lax.fori_loop(0, n_dev - 1, send_stats, 0)

    XB = 256

    def flip(i, carry):
        r = pl.ds(pl.multiple_of(i * XB, XB), XB)
        xt_v[r, :] = x_v[:, r].T
        return carry

    lax.fori_loop(0, H // XB, flip, 0)
    rest = all_v.at[pl.ds(0, n_dev - 1)]
    everybody = pltpu.make_async_remote_copy(
        src_ref=rest, dst_ref=rest, send_sem=st_ssem, recv_sem=st_rsem,
        device_id={'tp': partner}, device_id_type=MESH)
    everybody.wait_recv()

    loss = jnp.zeros((1, 1), F32)
    for b in range(T // LANES):
        m = all_v[:, 4 * b, :]
        s = all_v[:, 4 * b + 1, :]
        zt = jnp.sum(all_v[:, 4 * b + 2, :], axis=0, keepdims=True)
        M = jnp.max(m, axis=0, keepdims=True)
        S = jnp.sum(s * jnp.exp(m - M), axis=0, keepdims=True)
        loss = loss + jnp.sum(M + jnp.log(S) - zt, axis=1, keepdims=True)
        f = jnp.exp(msg_v[4 * b:4 * b + 1, :] - M) / (S * T)
        f_v[b * LANES:(b + 1) * LANES, :] = jnp.broadcast_to(f, (LANES, LANES)).T
    L_ref[...] = loss / T

    def grads(i, carry):
        r = pl.ds(pl.multiple_of(i * SB, SB), SB)
        hit = jnp.where(cols_f == lab_v[r, 0:1], 1.0 / T, 0.0)
        g_v[r, :] = (z_v[r, :] * f_v[r, 0:1] - hit).astype(BF16)
        return carry

    lax.fori_loop(0, T // SB, grads, 0)

    sent = []

    def rcopy(src, dst, to):
        i = len(sent)
        d = pltpu.make_async_remote_copy(src_ref=src, dst_ref=dst, send_sem=ssem.at[i], recv_sem=rsem.at[i],
                                         device_id={'tp': to}, device_id_type=MESH)
        d.start()
        sent.append(d)
        return d

    def unit(k, lo=0, n=U):
        return pl.ds(pl.multiple_of(k * U + lo, LANES), n)

    def part(s, k, core):
        wr = pl.ds(pl.multiple_of(core * HC + k * U, U), U)
        return lax.dot_general(g_v[s * R:(s + 1) * R, :], w_v[wr, :], NT, preferred_element_type=F32)

    DB = H // 8

    def dw_rows(lo, hi):
        def step(i, carry):
            r = pl.ds(pl.multiple_of(i * DB, DB), DB)
            dw_v[r, :] = jnp.dot(xt_v[r, :], g_v[...], preferred_element_type=F32).astype(BF16)
            return carry

        lax.fori_loop(lo, hi, step, 0)

    pair = {}

    def produce(off):
        for s in (0, 1):
            k = wrap(first[s] + off)
            ds[s, :, unit(k)] = part(s, k, 1 - c)
            pair[s, off] = rcopy(ds.at[s, :, unit(k)], dr.at[s, :, unit(k)], partner)
        for s in (0, 1):
            k = wrap(first[s] + off)
            own[s, :, unit(k)] = part(s, k, c)

    def join(s, off):
        k = wrap(first[s] + off)
        pair[s, off].wait_recv()
        own[s, :, unit(k)] += dr[s, :, unit(k)]

    one = {}
    produce(2)
    produce(1)
    for s in (0, 1):
        join(s, 2)
        k = wrap(first[s] + 2)
        one[s, 0] = rcopy(own.at[s, :, unit(k, 0, UH)], r1.at[s, 0], near1(s, 1))
        one[s, 1] = rcopy(own.at[s, :, unit(k, UH, UH)], r1.at[s, 1], near1(s, side - 1))
    produce(3)
    for s in (0, 1):
        join(s, 1)
        k = wrap(first[s] + 1)
        one[s, 2] = rcopy(own.at[s, :, unit(k, UH, UH)], r2.at[s, 0, :, UH:U], near1(s, 1))
    produce(0)
    for s in (0, 1):
        join(s, 3)
        k = wrap(first[s] + 3)
        one[s, 3] = rcopy(own.at[s, :, unit(k, 0, UH)], r2.at[s, 1, :, 0:UH], near1(s, side - 1))
    for s in (0, 1):
        join(s, 0)
    dw_rows(0, 4)
    for s in (0, 1):
        kp = wrap(first[s] + 1)
        km = wrap(first[s] + 3)
        one[s, 0].wait_recv()
        own[s, :, unit(kp, 0, UH)] += r1[s, 0]
        one[s, 4] = rcopy(own.at[s, :, unit(kp, 0, UH)], r2.at[s, 0, :, 0:UH], near1(s, 1))
        one[s, 1].wait_recv()
        own[s, :, unit(km, UH, UH)] += r1[s, 1]
        one[s, 5] = rcopy(own.at[s, :, unit(km, UH, UH)], r2.at[s, 1, :, UH:U], near1(s, side - 1))

    dw_rows(4, 8)

    def col2(j):
        return pl.ds(pl.multiple_of(j * J, LANES), J)

    two = {}
    top, bot = slice(0, RH), slice(RH, R)
    for s in (0, 1):
        for i in (2, 3, 4, 5):
            one[s, i].wait_recv()
        q_v[s] = own[s, :, unit(first[s])] + r2[s, 0] + r2[s, 1]
        jo, jp, jm = (wrap(second[s] + d) for d in (2, 1, 3))
        two[s, 0] = rcopy(q_v.at[s, top, col2(jo)], t1.at[s, 0], near2(s, 1))
        two[s, 1] = rcopy(q_v.at[s, bot, col2(jo)], t1.at[s, 1], near2(s, side - 1))
        two[s, 2] = rcopy(q_v.at[s, bot, col2(jp)], t2.at[s, 0, bot], near2(s, 1))
        two[s, 3] = rcopy(q_v.at[s, top, col2(jm)], t2.at[s, 1, top], near2(s, side - 1))
    for s in (0, 1):
        jp, jm = (wrap(second[s] + d) for d in (1, 3))
        two[s, 0].wait_recv()
        q_v[s, top, col2(jp)] += t1[s, 0]
        two[s, 4] = rcopy(q_v.at[s, top, col2(jp)], t2.at[s, 0, top], near2(s, 1))
        two[s, 1].wait_recv()
        q_v[s, bot, col2(jm)] += t1[s, 1]
        two[s, 5] = rcopy(q_v.at[s, bot, col2(jm)], t2.at[s, 1, bot], near2(s, side - 1))

    def at2(s, j, half):
        rows = slice(s * R + half * RH, s * R + (half + 1) * RH)
        return dx_v.at[rows, pl.ds(pl.multiple_of(c * HC + first[s] * U + j * J, LANES), J)]

    def at1(s, k, half):
        return dx_v.at[s * R:(s + 1) * R, pl.ds(pl.multiple_of(c * HC + k * U + half * UH, LANES), UH)]

    def block(s, k):
        return pl.ds(pl.multiple_of(c * HC + k * U, LANES), U)

    three = {}
    for s in (0, 1):
        j = second[s]
        for i in (2, 3, 4, 5):
            two[s, i].wait_recv()
        total = q_v[s, :, col2(j)] + t2[s, 0] + t2[s, 1]
        dx_v[s * R:(s + 1) * R, pl.ds(pl.multiple_of(c * HC + first[s] * U + j * J, LANES), J)] = total.astype(BF16)
        three[s, 0] = rcopy(at2(s, j, 0), at2(s, j, 0), near2(s, 1))
        three[s, 1] = rcopy(at2(s, j, 1), at2(s, j, 1), near2(s, side - 1))
        three[s, 2] = rcopy(at2(s, j, 1), at2(s, j, 1), near2(s, 1))
        three[s, 3] = rcopy(at2(s, j, 0), at2(s, j, 0), near2(s, side - 1))
    for s in (0, 1):
        jp, jm = (wrap(second[s] + d) for d in (1, 3))
        three[s, 0].wait_recv()
        three[s, 4] = rcopy(at2(s, jm, 0), at2(s, jm, 0), near2(s, 1))
        three[s, 1].wait_recv()
        three[s, 5] = rcopy(at2(s, jp, 1), at2(s, jp, 1), near2(s, side - 1))

    four = {}
    pairs = []

    def share(s, k):
        ref = dx_v.at[s * R:(s + 1) * R, block(s, k)]
        pairs.append(rcopy(ref, ref, partner))

    for s in (0, 1):
        for i in (2, 3, 4, 5):
            three[s, i].wait_recv()
        k = first[s]
        four[s, 0] = rcopy(at1(s, k, 0), at1(s, k, 0), near1(s, 1))
        four[s, 1] = rcopy(at1(s, k, 1), at1(s, k, 1), near1(s, side - 1))
        four[s, 2] = rcopy(at1(s, k, 1), at1(s, k, 1), near1(s, 1))
        four[s, 3] = rcopy(at1(s, k, 0), at1(s, k, 0), near1(s, side - 1))
        share(s, k)
    for s in (0, 1):
        kp, km = (wrap(first[s] + d) for d in (1, 3))
        four[s, 0].wait_recv()
        four[s, 4] = rcopy(at1(s, km, 0), at1(s, km, 0), near1(s, 1))
        four[s, 1].wait_recv()
        four[s, 5] = rcopy(at1(s, kp, 1), at1(s, kp, 1), near1(s, side - 1))
    for s in (0, 1):
        four[s, 2].wait_recv()
        share(s, wrap(first[s] + 3))
        four[s, 3].wait_recv()
        share(s, wrap(first[s] + 1))
    for s in (0, 1):
        four[s, 4].wait_recv()
        four[s, 5].wait_recv()
        share(s, wrap(first[s] + 2))
    for d in pairs:
        d.wait_recv()

    everybody.wait_send()
    for d in sent:
        d.wait_send()


N_COPIES = 8 + 4 * 12 + 8
N_PUT = 8


def put_kernel(l_ref, dw_ref, dx_ref, l_hbm, dw_hbm, dx_hbm, sem):
    n = dw_ref.shape[0] // N_PUT
    copies = [pltpu.make_async_copy(dw_ref.at[i * n:(i + 1) * n], dw_hbm.at[i * n:(i + 1) * n], sem.at[i])
              for i in range(N_PUT)]
    copies.append(pltpu.make_async_copy(dx_ref, dx_hbm, sem.at[N_PUT]))
    copies.append(pltpu.make_async_copy(l_ref, l_hbm, sem.at[N_PUT + 1]))
    for d in copies:
        d.start()
    for d in copies:
        d.wait()


def solution(mesh):
    n_dev = mesh.shape['tp']
    side = math.isqrt(n_dev // CORES)

    def local(X, W, labels):
        T, H = X.shape
        V = W.shape[1]
        R, HC = T // 2, H // CORES
        U = HC // side
        J = U // side
        vmem = pl.BlockSpec(memory_space=pltpu.VMEM)
        hbm = pl.BlockSpec(memory_space=pltpu.HBM)
        L, dW, dX = pl.pallas_call(
            functools.partial(head_kernel, n_dev, side),
            name='head',
            out_shape=(pltpu.VMEM((1, 1), F32), pltpu.VMEM((H, V), BF16), pltpu.VMEM((T, H), BF16)),
            in_specs=[hbm, hbm, hbm],
            out_specs=(vmem, vmem, vmem),
            scratch_shapes=[
                pltpu.VMEM((T, H), BF16), pltpu.VMEM((H, V), BF16), pltpu.VMEM((H, T), BF16), pltpu.VMEM((T, V), F32),
                pltpu.VMEM((1, T), jnp.int32),
                pltpu.VMEM((T, LANES), F32), pltpu.VMEM((T, LANES), F32), pltpu.VMEM((T, LANES), F32),
                pltpu.VMEM((8, LANES), F32), pltpu.VMEM((n_dev, 8, LANES), F32), pltpu.VMEM((T, V), BF16),
                pltpu.VMEM((2, R, HC), F32), pltpu.VMEM((2, R, HC), F32), pltpu.VMEM((2, R, HC), F32),
                pltpu.VMEM((2, 2, R, U // 2), F32), pltpu.VMEM((2, 2, R, U), F32), pltpu.VMEM((2, R, U), F32),
                pltpu.VMEM((2, 2, R // 2, J), F32), pltpu.VMEM((2, 2, R, J), F32),
                pltpu.SemaphoreType.DMA((2,)), pltpu.SemaphoreType.DMA((4,)),
                pltpu.SemaphoreType.DMA, pltpu.SemaphoreType.DMA,
                pltpu.SemaphoreType.DMA((N_COPIES,)), pltpu.SemaphoreType.DMA((N_COPIES,)),
            ],
            compiler_params=pltpu.CompilerParams(collective_id=0, has_side_effects=True,
                                                 vmem_limit_bytes=40 * 1024 * 1024),
        )(*(pltpu.with_memory_space_constraint(a, pltpu.HBM) for a in (X, W, labels.reshape(1, T))))

        L, dW, dX = pl.pallas_call(
            put_kernel,
            name='put',
            out_shape=(jax.ShapeDtypeStruct((1, 1), F32), jax.ShapeDtypeStruct((H, V), BF16),
                       jax.ShapeDtypeStruct((T, H), BF16)),
            in_specs=[vmem, vmem, vmem],
            out_specs=(hbm, hbm, hbm),
            scratch_shapes=[pltpu.SemaphoreType.DMA((N_PUT + 2,))],
            compiler_params=pltpu.CompilerParams(vmem_limit_bytes=1024 * 1024),
        )(*(pltpu.with_memory_space_constraint(a, pltpu.VMEM) for a in (L, dW, dX)))
        return L.reshape(1), dW, dX

    return jax.shard_map(local, mesh=mesh,
                         in_specs=(P('dp', None), P(None, 'tp'), P('dp')),
                         out_specs=(P('dp'), P('dp', 'tp'), P('dp', None)),
                         check_vma=False)
```
